32 devices in a mesh: section: 4 (over z), ctx: 8 (over y, x, core).
Axes of the slice: x: 2, y: 2, z: 4, core: 2. Of those that a mesh axis runs over, the one named last changes fastest.
Arguments:
- queries: bfloat16 [4, 1024, 4096], P('section', 'ctx'), may hold values from -130 to 130
- keys_new: bfloat16 [4, 1024, 1024], P('section', 'ctx'), may hold values from -6 to 6
- values_new: bfloat16 [4, 1024, 1024], P('section', 'ctx'), may hold values from -6 to 6
- stretch_cache: bfloat16 [4, 512, 2048], P('section'), may hold values from -6 to 6
- hadamard_signs: int32 [4, 2, 128], P('section'), may hold values from -1 to 1, as said below
- stretch_docs: int32 [8], replicated, may hold values from 0 to 1, never falling along the last dimension, each value on 1 to 5 neighbouring positions
Outputs:
- handed: bfloat16 [4, 1024, 4096], P('section', 'ctx')
The draws below stay inside these ranges and needn't reach their ends.
Inputs may be any that keep to these rules, and one draw needn't show every extreme that they name: `hadamard_signs`: each entry is -1 or 1. `stretch_docs`: never falling along the stretches; each document covers 1 to 5 stretches in a row.
All inputs are finite; a program needn't handle non-finite values.
Results may differ from the reference program's by a relative error of at most 0.0099.
Values may be sent and summed in bfloat16 or wider, within the bound.
A program may use at most 128 MiB of HBM per device.

```python
import math
import jax
import jax.numpy as jnp
import numpy as np
from jax import lax

QH = 32
KVH = 8
HD = 128
ROWS = 128
CACHE = 256
SECTIONS = 4
STRETCHES = 8
TOKENS = 1024
SPAN = 5
DOCS = 2
N_CTX = 8


def draw_queries(key, part):
    first_key = jax.random.fold_in(jax.random.fold_in(key, 11), 0)
    shape_all = (SECTIONS, TOKENS, QH * HD)
    base = jnp.clip(2.5 * jax.random.normal(first_key, shape_all, jnp.float32), -10.0, 10.0)
    return base.astype(jnp.bfloat16)


def draw_hadamard_signs(key, part):
    picks = jax.random.randint(jax.random.fold_in(key, 23), (SECTIONS, 2, HD), 0, 2)
    return (2 * picks - 1).astype(jnp.int32)


def shard_levels(own_key, extent, cuts, smallest, largest):
    def one(axis_at, shards_of):
        heights = jax.random.uniform(jax.random.fold_in(jax.random.fold_in(own_key, 6), axis_at), (shards_of,), jnp.float32, smallest / len(cuts), largest / len(cuts))
        return jnp.repeat(jnp.exp(heights), extent[axis_at] // shards_of).reshape((-1,) + (1,) * (len(extent) - axis_at - 1))

    gain = one(*cuts[0])
    for cut in cuts[1:]:
        gain = gain * one(*cut)
    return gain


def length_profile(number_of, total, reach, slope):
    loads = [(1 << 20) // math.isqrt(rank ** slope) + 1 for rank in range(2, number_of + 1)]
    surplus, holding = total - reach - (number_of - 1), [1] * (number_of - 1)
    while surplus > 0:
        movable = [i for i in range(number_of - 1) if holding[i] < reach]
        whole, left = sum([loads[i] for i in movable]), surplus
        for i in movable:
            extra = min(reach - holding[i], max(1, left * loads[i] // whole), surplus)
            holding[i] = holding[i] + extra
            surplus = surplus - extra
    return np.array([reach] + holding)


def uneven(key, number_of, total, most, slope):
    if number_of == 2:
        one = jax.random.randint(key, (), max(1, total - most), min(most, total - 1) + 1)
        return jnp.stack([one, total - one])
    tallies = jnp.asarray(length_profile(number_of, total, most, slope), jnp.int32)
    pairs = (number_of - 1) // 2
    donor, sink = tallies[1:1 + 2 * pairs:2], tallies[2:2 + 2 * pairs:2]
    room = jnp.minimum(donor - 1, most - sink)
    passed = jax.random.randint(jax.random.fold_in(key, 1), (pairs,), 0, 1 << 20) % (room + 1)
    tallies = tallies.at[1:1 + 2 * pairs:2].set(donor - passed).at[2:2 + 2 * pairs:2].set(sink + passed)
    return tallies[jax.random.permutation(jax.random.fold_in(key, 2), number_of)]


def centred(rng, extent, width, reach, cuts=(), kind=jnp.bfloat16):
    values = width * jax.random.normal(rng, extent, jnp.float32)
    if cuts:
        values = values * shard_levels(rng, extent, cuts, -0.22, 0.18)
    return jnp.clip(values, -reach, reach).astype(kind)


def setup_inputs(seed: int = 0) -> dict:
    arg_keys = jax.random.split(jax.random.key(seed), 7)
    return {
        "queries": draw_queries(jax.random.fold_in(arg_keys[6], 71), 0),
        "keys_new": centred(arg_keys[1], (SECTIONS, TOKENS, KVH * HD), 1.0, 6.0, ((0, 4), (1, 8))),
        "values_new": centred(arg_keys[2], (SECTIONS, TOKENS, KVH * HD), 1.0, 6.0, ((0, 4), (1, 8))),
        "stretch_cache": centred(arg_keys[3], (SECTIONS, DOCS * CACHE, 2 * KVH * HD), 1.0, 6.0, ((0, 4),)),
        "hadamard_signs": draw_hadamard_signs(jax.random.fold_in(arg_keys[6], 71), 0),
        "stretch_docs": jnp.searchsorted(jnp.cumsum(uneven(arg_keys[5], DOCS, STRETCHES, SPAN, 0)), jnp.arange(STRETCHES), side="right").astype(jnp.int32),
    }


def hadamard(length):
    numbers = np.arange(length)
    common = numbers[:, None] & numbers[None, :]
    parity = np.zeros((length, length), np.int64)
    for bit_place in range(max(int(length).bit_length(), 1)):
        parity = parity ^ ((common >> bit_place) & 1)
    return 1.0 - 2.0 * parity


def rotate(source, sign_row, rotation):
    row_count = source.shape[0]
    head_size = rotation.shape[0]
    shaped = (source.reshape(row_count, -1, head_size) * sign_row.astype(source.dtype)).reshape(-1, head_size)
    turned = jnp.dot(shaped, rotation, preferred_element_type=jnp.float32) * (head_size ** -0.5)
    return turned.reshape(row_count, -1).astype(jnp.bfloat16)


def reference(queries, keys_new, values_new, stretch_cache, hadamard_signs, stretch_docs):
    rotation = jnp.asarray(hadamard(HD), dtype=jnp.bfloat16)
    inverse = jnp.asarray(hadamard(HD), dtype=jnp.float32)
    groups = QH // KVH

    def one_section(section_args):
        section_query, section_keys, section_values, section_cache, section_signs = section_args
        fronts = jnp.concatenate([rotate(section_keys, section_signs[0], rotation), rotate(section_values, section_signs[1], rotation)], axis=1)

        def one_stretch(stretch_index):
            query_rows = lax.dynamic_slice_in_dim(section_query, stretch_index * ROWS, ROWS, 0)
            query_turned = rotate(query_rows, section_signs[0], rotation).reshape(ROWS, KVH, groups, HD)
            doc_mine = stretch_docs[stretch_index]
            own_cache = lax.dynamic_slice_in_dim(section_cache, (doc_mine * CACHE).astype(jnp.int32), CACHE, 0)
            keyset = jnp.concatenate([own_cache, fronts], axis=0)
            key_part = keyset[:, :KVH * HD].reshape(-1, KVH, HD)
            value_part = keyset[:, KVH * HD:].reshape(-1, KVH, HD)
            scores = jnp.einsum("rkgd,nkd->rkgn", query_turned.astype(jnp.float32), key_part.astype(jnp.float32)) * (HD ** -0.5)
            position = jnp.arange(TOKENS, dtype=jnp.int32)
            key_stretch = position // ROWS
            key_row = position % ROWS
            query_row = jnp.arange(ROWS, dtype=jnp.int32)
            doc_keys = stretch_docs[key_stretch]
            same_stretch = (key_stretch[None, :] == stretch_index) & (key_row[None, :] <= query_row[:, None])
            earlier = (key_stretch[None, :] < stretch_index) & (doc_keys[None, :] == doc_mine)
            allowed = jnp.concatenate([jnp.ones((ROWS, CACHE), dtype=bool), same_stretch | earlier], axis=1)
            scores = jnp.where(allowed[:, None, None, :], scores, -jnp.inf)
            row_max = scores.max(-1, keepdims=True)
            exponent = jnp.exp(scores - row_max)
            row_sum = exponent.sum(-1)
            weights = exponent.astype(jnp.bfloat16)
            averaged = jnp.einsum("rkgn,nkd->rkgd", weights.astype(jnp.float32), value_part.astype(jnp.float32)) / row_sum[..., None]
            restored = jnp.dot(averaged.reshape(-1, HD), inverse, precision=lax.Precision.HIGHEST)
            restored = restored * (HD ** -0.5) * section_signs[1].astype(jnp.float32)
            return restored.reshape(ROWS, QH * HD).astype(jnp.bfloat16)

        return lax.map(one_stretch, jnp.arange(N_CTX, dtype=jnp.int32)).reshape(TOKENS, QH * HD)

    heads_out = lax.map(one_section, (queries, keys_new, values_new, stretch_cache, hadamard_signs))
    return jnp.roll(heads_out, 1, axis=0)
```

```python
import functools

import jax
import jax.numpy as jnp
import numpy as np
from jax import lax
from jax.experimental import pallas as pl
from jax.experimental.pallas import tpu as pltpu
from jax.sharding import PartitionSpec as P

CACHE = 256
MESH = pl.DeviceIdType.MESH


def hadamard(length):
    numbers = np.arange(length)
    common = numbers[:, None] & numbers[None, :]
    parity = np.zeros((length, length), np.int64)
    for bit_place in range(max(int(length).bit_length(), 1)):
        parity = parity ^ common >> bit_place & 1
    return 1.0 - 2.0 * parity


def attention_kernel(
    n,
    sections,
    docs_ref,
    signs_ref,
    hada_ref,
    q_hbm,
    k_hbm,
    v_hbm,
    cache_hbm,
    out_hbm,
    q_buf,
    cache_buf,
    own,
    held,
    out_buf,
    load_sem,
    own_sem,
    send_sem,
    recv_sem,
    out_send,
    out_recv,
):
    section = lax.axis_index("section")
    me = lax.axis_index("ctx")
    odd = lax.rem(me, 2)
    reach = held.shape[0]
    half = reach // 2
    heads = own.shape[0]
    rows, hd = own.shape[2], own.shape[3]
    width = out_buf.shape[2]
    groups = width // hd
    kv_width = heads * hd
    detour = n == 8

    def cols(start, size):
        return pl.ds(pl.multiple_of(start, hd), size)

    def own_copies(h):
        return (
            pltpu.make_async_copy(k_hbm.at[:, cols(h * hd, hd)], own.at[h, 0], own_sem.at[h, 0]),
            pltpu.make_async_copy(v_hbm.at[:, cols(h * hd, hd)], own.at[h, 1], own_sem.at[h, 1]),
        )

    def start_own(h, carry):
        for copy in own_copies(h):
            copy.start()
        return carry

    lax.fori_loop(0, heads, start_own, 0)
    cache_copy = pltpu.make_async_copy(cache_hbm, cache_buf, load_sem.at[0])
    cache_copy.start()
    q_copy = pltpu.make_async_copy(q_hbm, q_buf, load_sem.at[1])
    q_copy.start()

    barrier = pltpu.get_barrier_semaphore()
    sibling = me + 1 - 2 * odd
    following = lax.rem(section + 1, sections)
    previous = lax.rem(section + sections - 1, sections)

    def greet(sec, ctx):
        pl.semaphore_signal(barrier, inc=1, device_id=(sec, ctx), device_id_type=MESH)

    greet(section, sibling)
    greet(following, me)
    greet(previous, me)
    count = jnp.int32(3)
    for e in range(2, reach + 1, 2):
        @pl.when(me + e < n)
        def _(e=e):
            greet(section, me + e)

        @pl.when(me >= e)
        def _(e=e):
            greet(section, me - e)

        count = count + jnp.where(me + e < n, 1, 0) + jnp.where(me >= e, 1, 0)
    pl.semaphore_wait(barrier, count)

    def remote(src, row, h, target, distance):
        return pltpu.make_async_remote_copy(
            src_ref=src,
            dst_ref=held.at[distance - 1, h],
            send_sem=send_sem.at[row, h],
            recv_sem=recv_sem.at[distance - 1, h],
            device_id=(section, target),
            device_id_type=MESH,
        )

    def own_sends(h, act):
        for e in range(2, reach + 1, 2):
            go = me + e < n
            if detour and e == 2:
                go = go & (me // 2 != 1)

            @pl.when(go)
            def _(e=e):
                act(remote(own.at[h], e // 2 - 1, h, me + e, e))

        @pl.when(odd == 0)
        def _():
            act(remote(own.at[h], half, h, me + 1, 1))

    def relay_sends(h, act, wait):
        for e in range(reach, 1, -2):
            @pl.when(me >= e)
            def _(e=e):
                block = held.at[e - 1, h]
                if wait:
                    remote(block, 0, h, me, e).wait_recv()
                if detour and e == 4:
                    @pl.when(me >= n - 2)
                    def _():
                        act(remote(block, reach + 1, h, me - 2, 2))

                @pl.when(odd == 1)
                def _():
                    act(remote(block, half + e // 2, h, me - 1, e - 1))

                if e < reach:
                    @pl.when(odd == 0)
                    def _():
                        act(remote(block, half + e // 2, h, me + 1, e + 1))

    def send_own(h, carry):
        for copy in own_copies(h):
            copy.wait()
        own_sends(h, lambda copy: copy.start())
        return carry

    lax.fori_loop(0, heads, send_own, 0)

    for d in range(1, reach + 1):
        @pl.when(me < d)
        def _(d=d):
            held[d - 1] = jnp.zeros(held.shape[1:], held.dtype)

    my_doc = docs_ref[me]
    biases = []
    for d in range(1, reach + 1):
        seen = (me >= d) & (docs_ref[jnp.maximum(me - d, 0)] == my_doc)
        biases.append(jnp.where(seen, 0.0, -jnp.inf).astype(jnp.float32))
    picks = [
        jnp.full((1, hd), jnp.where(my_doc == doc, 1.0, 0.0), jnp.float32).astype(jnp.bfloat16)
        for doc in range(cache_buf.shape[0] // CACHE)
    ]

    def cache_block(start):
        terms = [
            cache_buf[doc * CACHE : (doc + 1) * CACHE, cols(start, hd)] * pick
            for doc, pick in enumerate(picks)
        ]
        return functools.reduce(jnp.add, terms)

    root = hd ** -0.5
    sign_k = signs_ref[0:1, :].astype(jnp.float32) * root
    sign_v = signs_ref[1:2, :].astype(jnp.float32) * root
    hada = hada_ref[...]
    factor = root * float(np.log2(np.e))
    cache_copy.wait()
    q_copy.wait()
    relay_sends(0, lambda copy: copy.start(), True)

    def out_copy(h):
        return pltpu.make_async_remote_copy(
            src_ref=out_buf.at[h],
            dst_ref=out_hbm.at[:, cols(h * width, width)],
            send_sem=out_send.at[h],
            recv_sem=out_recv.at[h],
            device_id=(following, me),
            device_id_type=MESH,
        )

    causal = lax.broadcasted_iota(jnp.int32, (rows, rows), 1) <= lax.broadcasted_iota(
        jnp.int32, (rows, rows), 0
    )

    def head_step(h, carry):
        back_k = jnp.dot(cache_block(h * hd), hada, preferred_element_type=jnp.float32)
        back_v = jnp.dot(cache_block(kv_width + h * hd), hada, preferred_element_type=jnp.float32)
        back_k = (back_k * sign_k).astype(jnp.bfloat16)
        back_v = (back_v * sign_v).astype(jnp.bfloat16)
        for d in range(1, reach + 1, 2):
            @pl.when(me >= d)
            def _(d=d):
                remote(held.at[d - 1, h], 0, h, me, d).wait_recv()
        keys = jnp.concatenate(
            [back_k, own[h, 0]] + [held[d, h, 0] for d in range(reach)], axis=0
        )
        values = jnp.concatenate(
            [back_v, own[h, 1]] + [held[d, h, 1] for d in range(reach)], axis=0
        )
        for g in range(groups):
            if g == groups // 2:
                @pl.when(h + 1 < heads)
                def _():
                    relay_sends(h + 1, lambda copy: copy.start(), True)
            query = q_buf[:, cols(h * width + g * hd, hd)]
            scores = lax.dot_general(
                query, keys, (((1,), (1,)), ((), ())), preferred_element_type=jnp.float32
            )
            parts = [scores[:, at : at + rows] for at in range(0, CACHE, rows)]
            parts.append(jnp.where(causal, scores[:, CACHE : CACHE + rows], -jnp.inf))
            for d in range(reach):
                at = CACHE + rows * (d + 1)
                parts.append(scores[:, at : at + rows] + biases[d])
            top = functools.reduce(jnp.maximum, parts)
            top = jnp.max(top, axis=1, keepdims=True)
            expo = [jnp.exp2((part - top) * factor) for part in parts]
            total = jnp.sum(functools.reduce(jnp.add, expo), axis=1, keepdims=True)
            weights = jnp.concatenate([part.astype(jnp.bfloat16) for part in expo], axis=1)
            summed = jnp.dot(weights, values, preferred_element_type=jnp.float32)
            out_buf[h, :, g * hd : (g + 1) * hd] = (summed / total).astype(out_buf.dtype)
        out_copy(h).start()
        return carry

    lax.fori_loop(0, heads, head_step, 0)

    def finish(h, carry):
        own_sends(h, lambda copy: copy.wait_send())
        relay_sends(h, lambda copy: copy.wait_send(), False)
        out_copy(h).wait()
        return carry

    lax.fori_loop(0, heads, finish, 0)


def per_device(n, sections, queries, keys_new, values_new, stretch_cache, signs, docs):
    rows, q_width = queries.shape[1:]
    kv_width = keys_new.shape[-1]
    hd = signs.shape[-1]
    heads = kv_width // hd
    width = q_width // heads
    reach = n // 2
    dtype = queries.dtype
    anywhere = pl.BlockSpec(memory_space=pl.ANY)
    vmem = pl.BlockSpec(memory_space=pltpu.VMEM)
    out = pl.pallas_call(
        functools.partial(attention_kernel, n, sections),
        out_shape=jax.ShapeDtypeStruct((rows, q_width), dtype),
        in_specs=[pl.BlockSpec(memory_space=pltpu.SMEM), vmem, vmem] + [anywhere] * 4,
        out_specs=anywhere,
        scratch_shapes=[
            pltpu.VMEM((rows, q_width), dtype),
            pltpu.VMEM(stretch_cache.shape[1:], dtype),
            pltpu.VMEM((heads, 2, rows, hd), dtype),
            pltpu.VMEM((reach, heads, 2, rows, hd), dtype),
            pltpu.VMEM((heads, rows, width), dtype),
            pltpu.SemaphoreType.DMA((2,)),
            pltpu.SemaphoreType.DMA((heads, 2)),
            pltpu.SemaphoreType.DMA((reach + 2, heads)),
            pltpu.SemaphoreType.DMA((reach, heads)),
            pltpu.SemaphoreType.DMA((heads,)),
            pltpu.SemaphoreType.DMA((heads,)),
        ],
        compiler_params=pltpu.CompilerParams(
            collective_id=0, has_side_effects=True, vmem_limit_bytes=60 * 1024 * 1024
        ),
    )(
        docs,
        signs[0],
        jnp.asarray(hadamard(hd), dtype),
        queries[0],
        keys_new[0],
        values_new[0],
        stretch_cache[0],
    )
    return out[None]


def solution(mesh):
    in_specs = (
        P("section", "ctx", None),
        P("section", "ctx", None),
        P("section", "ctx", None),
        P("section", None, None),
        P("section", None, None),
        P(),
    )
    out_specs = P("section", "ctx", None)
    body = functools.partial(per_device, mesh.shape["ctx"], mesh.shape["section"])
    return jax.shard_map(body, mesh=mesh, in_specs=in_specs, out_specs=out_specs, check_vma=False)
```
